128 devices in a mesh: gx: 8 (over x, core), gy: 16 (over y, z).
Axes of the slice: x: 4, y: 4, z: 4, core: 2. Of those that a mesh axis runs over, the one named last changes fastest.
Arguments:
- hot_ids: int32 [1048576], P(('gx', 'gy')), may hold values from 0 to 2047
- hot_grads: bfloat16 [1048576, 128], P(('gx', 'gy')), may hold values from -6 to 6
- cold_grads: bfloat16 [8, 16, 16, 512, 128], P('gx', 'gy'), may hold values from -6 to 6
- cold_slots: int32 [8, 16, 16, 512], P('gx', 'gy'), may hold values from 0 to 2047
- cold_counts: int32 [8, 16, 16], P('gx', 'gy'), may hold values from 1 to 512, as said below
Outputs:
- hot_grad: float32 [2048, 128], replicated
- cold_grad: float32 [8, 32768, 128], P('gx', 'gy')
The draws below stay inside these ranges and needn't reach their ends.
Inputs may be any that keep to these rules, and one draw needn't show every extreme that they name: In each group g, some owner d receives cold_counts[g, s, d] = 512 from every s; loads per owner are skewed.
All inputs are finite; a program needn't handle non-finite values.
Results may differ from the reference program's by a relative error of at most 0.0003.
Values may be sent and summed in bfloat16 or wider, within the bound.
A program may use at most 64 MiB of HBM per device.

```python
import jax
import jax.numpy as jnp
from jax import lax

D = 128
HOT = 2048
LOOK = 8192
CAP = 512
OWN_ROWS = 2048
LOOKUPS = 1048576
N_GX = 8
N_GY = 16


def draw_cold_counts(key, part):
    first = jax.random.fold_in(key, 11)
    second = jax.random.fold_in(key, 12)
    third = jax.random.fold_in(key, 13)
    limits = jax.random.randint(first, (N_GX, 1, N_GY), 1, CAP + 1)
    counts = jax.random.randint(second, (N_GX, N_GY, N_GY), 1, CAP + 1)
    counts = jnp.minimum(counts, limits)
    heavy = jax.random.randint(third, (N_GX, 1, 1), 0, N_GY)
    owners = jnp.arange(N_GY, dtype=jnp.int32)[None, None, :]
    return jnp.where(owners == heavy, CAP, counts).astype(jnp.int32)


def with_ends(values, rng, least, high):
    dims = values.shape
    spot = [jax.random.randint(jax.random.fold_in(rng, axis), (), 0, dims[axis]) for axis in range(len(dims))]
    values = values.at[tuple(spot)].set(least)
    longest = dims.index(max(dims))
    spot[longest] = (spot[longest] + 1) % dims[longest]
    return values.at[tuple(spot)].set(high)


def block_levels(rng, dims, shards, low, top_value):
    def one(dim, blocks):
        steps = jax.random.uniform(jax.random.fold_in(jax.random.fold_in(rng, 6), dim), (blocks,), jnp.float32, low / len(shards), top_value / len(shards))
        return jnp.repeat(jnp.exp(steps), dims[dim] // blocks).reshape((-1,) + (1,) * (len(dims) - dim - 1))

    gain = one(*shards[0])
    for cut in shards[1:]:
        gain = gain * one(*cut)
    return gain


def scatter_about(own_key, shape, spread, bound, split=(), kind=jnp.bfloat16):
    gain = block_levels(own_key, shape, split, -0.22, 0.18) if split else 1.0
    result = jax.random.normal(own_key, shape, jnp.float32) * spread * gain
    return jnp.minimum(jnp.maximum(result, -bound), bound).astype(kind)


def setup_inputs(seed: int = 0) -> dict:
    arg_keys = jax.random.split(jax.random.key(seed), 6)
    hot_ids = with_ends(jax.random.randint(arg_keys[0], (LOOKUPS,), 0, HOT), jax.random.fold_in(arg_keys[0], 1), 0, HOT - 1).astype(jnp.int32)
    hot_grads = scatter_about(arg_keys[1], (LOOKUPS, D), 1.0, 6.0, ((0, 128),))
    cold_grads = scatter_about(arg_keys[2], (N_GX, N_GY, N_GY, CAP, D), 1.0, 6.0, ((0, 8), (1, 16)))
    cold_slots = with_ends(jax.random.randint(arg_keys[3], (N_GX, N_GY, N_GY, CAP), 0, OWN_ROWS), jax.random.fold_in(arg_keys[3], 1), 0, OWN_ROWS - 1).astype(jnp.int32)
    cold_counts = draw_cold_counts(jax.random.fold_in(arg_keys[5], 71), 0)
    return dict(hot_ids=hot_ids, hot_grads=hot_grads, cold_grads=cold_grads, cold_slots=cold_slots, cold_counts=cold_counts)


def reference(hot_ids, hot_grads, cold_grads, cold_slots, cold_counts):
    hot_sum = jax.ops.segment_sum(hot_grads.astype(jnp.float32), hot_ids, num_segments=HOT)
    hot_grad = hot_sum * (HOT / (LOOK * N_GX * N_GY)) ** 0.5
    places = jnp.arange(CAP, dtype=jnp.int32)
    valid = places[None, None, None, :] < cold_counts[..., None]
    payload = jnp.where(valid[..., None], cold_grads, jnp.zeros_like(cold_grads))
    owners = jnp.arange(N_GY, dtype=jnp.int32)[None, None, :, None] * OWN_ROWS
    table_rows = (owners + cold_slots).astype(jnp.int32)

    def one_group(pair):
        rows_data, rows_index = pair
        return jax.ops.segment_sum(rows_data.reshape(-1, D).astype(jnp.float32), rows_index.reshape(-1), num_segments=OWN_ROWS * N_GY)

    cold_grad = lax.map(one_group, (payload, table_rows))
    return hot_grad, cold_grad
```

```python
import jax
import jax.numpy as jnp
from jax import lax
from jax.experimental import pallas as pl
from jax.experimental.pallas import tpu as pltpu
from jax.sharding import PartitionSpec as P

MESH = pl.DeviceIdType.MESH
BF16 = jnp.bfloat16
F32 = jnp.float32

ROWS = 2048
HALF = 1024
WIDTH = 128
LOOK = 8192
CAP = 512
GX, GY, NX, NY, NZ = 8, 16, 4, 4, 4

NEAR = sorted(
    [(a, b) for a in range(NY) for b in range(NZ)],
    key=lambda o: (min(o[0], NY - o[0]) + min(o[1], NZ - o[1]), o),
)


def selector_tile(local_ref, row, base, iota):
    halves = []
    for side in range(2):
        ids = local_ref[pl.ds(row + side, 1), :] - base
        ids = jnp.broadcast_to(ids, (16, WIDTH)).astype(BF16)
        halves.append(
            jnp.concatenate(
                [
                    jnp.where(ids == (iota + BF16(16 * i)), BF16(1), BF16(0))
                    for i in range(16)
                ],
                axis=0,
            )
        )
    return jnp.concatenate(halves, axis=1)


def split_by_bit(bits_t, column, grads):
    high = grads * jnp.broadcast_to(bits_t[:, column : column + 1], (128, WIDTH)).astype(BF16)
    return grads - high, high


def kernel(
    ids_hbm, hot_hbm, cold_hbm, slots_hbm, counts,
    hot, cold,
    ids, grads, wide, local, slots, masked,
    partial, from_core, to_x, from_x, mine, from_y, got, got_slots, cold_local, cold_wide,
    local_sem, core_s, core_r, x_s, x_r, ys_s, ys_r, yg_s, yg_r,
    xg_s, xg_r, cg_s, cg_r, row_s, row_r, slot_s, slot_r,
):
    gx, gy = lax.axis_index("gx"), lax.axis_index("gy")
    x, core = gx // 2, lax.rem(gx, 2)
    y, z = gy // NZ, lax.rem(gy, NZ)

    def along_y(k):
        dy, dz = NEAR[k]
        return lax.rem(y + dy, NY) * NZ + lax.rem(z + dz, NZ)

    def x_peer(step):
        return lax.rem(x + step, NX)

    def at_gy(owner):
        return {"gx": gx, "gy": owner}

    def at_x(column):
        return {"gx": column * 2 + core, "gy": gy}

    other_core = {"gx": x * 2 + (1 - core), "gy": gy}

    def remote(src, dst, send, recv, where):
        return pltpu.make_async_remote_copy(
            src_ref=src, dst_ref=dst, send_sem=send, recv_sem=recv,
            device_id=where, device_id_type=MESH,
        )

    load_slots = pltpu.make_async_copy(slots_hbm, slots, local_sem.at[0])
    load_ids = pltpu.make_async_copy(ids_hbm, ids, local_sem.at[1])
    load_grads = pltpu.make_async_copy(hot_hbm, grads, local_sem.at[2])
    load_own = pltpu.make_async_copy(cold_hbm.at[gy], got.at[0], local_sem.at[3])
    load_slots.start()
    load_ids.start()
    load_grads.start()
    load_own.start()

    barrier = pltpu.get_barrier_semaphore()
    for k in range(1, GY):
        pl.semaphore_signal(barrier, inc=1, device_id=at_gy(along_y(k)), device_id_type=MESH)
    for step in range(1, NX):
        pl.semaphore_signal(barrier, inc=1, device_id=at_x(x_peer(step)), device_id_type=MESH)
    pl.semaphore_signal(barrier, inc=1, device_id=other_core, device_id_type=MESH)

    load_slots.wait()
    place = lax.broadcasted_iota(jnp.int32, (1, WIDTH), 1)
    masked[...] = jnp.full_like(masked, -1)
    for d in range(GY):
        for i in range(CAP // WIDTH):
            piece = slots[d : d + 1, i * WIDTH : (i + 1) * WIDTH]
            masked[d, i : i + 1, :] = jnp.where(place + i * WIDTH < counts[0, d], piece, -1)

    load_ids.wait()
    local[...] = (ids[...] & (HALF - 1)).astype(F32)
    bits_t = jnp.transpose((ids[...] >> 10).astype(F32))
    load_grads.wait()
    for r in range(LOOK // 128):
        rows = slice(r * 128, (r + 1) * 128)
        low, high = split_by_bit(bits_t, r, grads[rows, :])
        wide[rows, 0:WIDTH] = low
        wide[rows, WIDTH:] = high

    pl.semaphore_wait(barrier, GY - 1 + NX - 1 + 1)

    def row_copy(k):
        owner = along_y(k)
        return remote(cold_hbm.at[owner], got.at[k], row_s.at[k], row_r.at[k], at_gy(owner))

    def slot_copy(k):
        owner = along_y(k)
        return remote(masked.at[owner], got_slots.at[k], slot_s.at[k], slot_r.at[k], at_gy(owner))

    for k in range(1, GY):
        slot_copy(k).start()
        row_copy(k).start()

    iota = lax.broadcasted_iota(jnp.int32, (16, WIDTH), 0).astype(F32).astype(BF16)

    def core_copy(s):
        return remote(
            partial.at[s, 1 - core], from_core.at[s], core_s.at[s], core_r.at[s], other_core
        )

    def x_copy(s):
        return remote(to_x.at[s], from_x.at[s], x_s.at[s], x_r.at[s], at_x(x_peer(3 - s)))

    def hot_block(s, carry):
        base = (x_peer(3 - s) * 256).astype(F32)
        total = None
        for t in range(LOOK // 256):
            product = jnp.dot(
                selector_tile(local, 2 * t, base, iota),
                wide[t * 256 : (t + 1) * 256, :],
                preferred_element_type=F32,
            )
            total = product if total is None else total + product
        partial[s, 0] = total[:, :WIDTH]
        partial[s, 1] = total[:, WIDTH:]
        core_copy(s).start()

        @pl.when(s > 0)
        def _():
            core_copy(s - 1).wait_recv()
            to_x[s - 1] = partial[s - 1, core] + from_core[s - 1]
            x_copy(s - 1).start()

        return carry

    lax.fori_loop(0, NX, hot_block, 0)

    def cold_block(k, slot_rows, first):
        cold_local[...] = jnp.where(slot_rows < 0, -1, slot_rows & (HALF - 1)).astype(F32)
        turned = jnp.transpose((slot_rows >> 10).astype(F32))
        for r in range(CAP // 128):
            rows = slice(r * 128, (r + 1) * 128)
            low, high = split_by_bit(turned, r, got[k, rows, :])
            cold_wide[rows, 0:WIDTH] = low
            cold_wide[rows, WIDTH:] = high
        for j in range(4):
            total = None
            for t in range(CAP // 256):
                product = jnp.dot(
                    selector_tile(cold_local, 2 * t, 256.0 * j, iota),
                    cold_wide[t * 256 : (t + 1) * 256, :],
                    preferred_element_type=F32,
                )
                total = product if total is None else total + product
            rows = slice(j * 256, (j + 1) * 256)
            if first:
                cold[0, rows, :] = total[:, :WIDTH]
                cold[1, rows, :] = total[:, WIDTH:]
            else:
                cold[0, rows, :] += total[:, :WIDTH]
                cold[1, rows, :] += total[:, WIDTH:]

    def cold_blocks(low, high):
        def body(k, carry):
            remote(got.at[k], got.at[k], row_s.at[k], row_r.at[k], other_core).wait_recv()
            remote(
                got_slots.at[k], got_slots.at[k], slot_s.at[k], slot_r.at[k], other_core
            ).wait_recv()
            cold_block(k, got_slots[k], False)
            return carry

        lax.fori_loop(low, high, body, 0)

    load_own.wait()
    cold_block(0, masked[gy], True)

    core_copy(3).wait_recv()
    own = partial[3, core] + from_core[3]
    for s in range(3):
        x_copy(s).wait_recv()
        own = own + from_x[s]
    mine[...] = own.reshape(GY, 16, WIDTH)

    def scatter_copy(k):
        owner = along_y(k)
        return remote(mine.at[owner], from_y.at[k], ys_s.at[k], ys_r.at[k], at_gy(owner))

    for k in range(1, GY):
        scatter_copy(k).start()

    cold_blocks(1, 4)

    block = core * NX + x
    sum16 = mine[gy]
    for k in range(1, GY):
        scatter_copy(k).wait_recv()
        sum16 = sum16 + from_y[k]
    hot[block, gy] = sum16

    def gather_copy(k):
        return remote(
            hot.at[block, gy], hot.at[block, gy], yg_s.at[k], yg_r.at[k], at_gy(along_y(k))
        )

    for k in range(1, GY):
        gather_copy(k).start()

    cold_blocks(4, 7)

    for k in range(1, GY):
        gather_copy(k).wait_recv()

    def x_spread(step):
        return remote(
            hot.at[block], hot.at[block], xg_s.at[step], xg_r.at[step], at_x(x_peer(step))
        )

    def core_spread(step):
        piece = core * NX + x_peer(step)
        return remote(hot.at[piece], hot.at[piece], cg_s.at[step], cg_r.at[step], other_core)

    for step in range(1, NX):
        x_spread(step).start()
    core_spread(0).start()

    cold_blocks(7, 12)

    for step in range(1, NX):
        x_spread(step).wait_recv()
        piece = core * NX + x_peer(NX - step)
        remote(hot.at[piece], hot.at[piece], cg_s.at[step], cg_r.at[step], other_core).start()

    cold_blocks(12, GY)

    for step in range(NX):
        core_spread(step).wait_recv()

    for k in range(1, GY):
        slot_copy(k).wait_send()
        row_copy(k).wait_send()
        scatter_copy(k).wait_send()
        gather_copy(k).wait_send()
    for s in range(NX):
        core_copy(s).wait_send()
        core_spread(s).wait_send()
    for s in range(3):
        x_copy(s).wait_send()
        x_spread(s + 1).wait_send()


def per_device(hot_ids, hot_grads, cold_grads, cold_slots, cold_counts):
    factor = (ROWS / (LOOK * GX * GY)) ** 0.5
    in_hbm = pl.BlockSpec(memory_space=pltpu.HBM)
    in_vmem = pl.BlockSpec(memory_space=pltpu.VMEM)
    dma = pltpu.SemaphoreType.DMA
    hot, cold = pl.pallas_call(
        kernel,
        name="table_grads",
        out_shape=(
            jax.ShapeDtypeStruct((GX, GY, 16, WIDTH), F32),
            jax.ShapeDtypeStruct((2, HALF, WIDTH), F32),
        ),
        in_specs=[in_hbm] * 4 + [pl.BlockSpec(memory_space=pltpu.SMEM)],
        out_specs=[in_vmem] * 2,
        scratch_shapes=[
            pltpu.VMEM((LOOK // WIDTH, WIDTH), jnp.int32),
            pltpu.VMEM((LOOK, WIDTH), BF16),
            pltpu.VMEM((LOOK, 2 * WIDTH), BF16),
            pltpu.VMEM((LOOK // WIDTH, WIDTH), F32),
            pltpu.VMEM((GY, CAP), jnp.int32),
            pltpu.VMEM((GY, 8, WIDTH), jnp.int32),
            pltpu.VMEM((NX, 2, 256, WIDTH), F32),
            pltpu.VMEM((NX, 256, WIDTH), F32),
            pltpu.VMEM((3, 256, WIDTH), F32),
            pltpu.VMEM((3, 256, WIDTH), F32),
            pltpu.VMEM((GY, 16, WIDTH), F32),
            pltpu.VMEM((GY, 16, WIDTH), F32),
            pltpu.VMEM((GY, CAP, WIDTH), BF16),
            pltpu.VMEM((GY, 8, WIDTH), jnp.int32),
            pltpu.VMEM((8, WIDTH), F32),
            pltpu.VMEM((CAP, 2 * WIDTH), BF16),
            dma((4,)),
            dma((NX,)), dma((NX,)),
            dma((3,)), dma((3,)),
            dma((GY,)), dma((GY,)),
            dma((GY,)), dma((GY,)),
            dma((NX,)), dma((NX,)),
            dma((NX,)), dma((NX,)),
            dma((GY,)), dma((GY,)),
            dma((GY,)), dma((GY,)),
        ],
        compiler_params=pltpu.CompilerParams(
            collective_id=0, has_side_effects=True, vmem_limit_bytes=48 * 2**20
        ),
    )(
        hot_ids.reshape(LOOK // WIDTH, WIDTH),
        hot_grads,
        cold_grads.reshape(GY, CAP, WIDTH),
        cold_slots.reshape(GY, CAP),
        cold_counts.reshape(1, GY),
    )
    return hot.reshape(ROWS, WIDTH) * factor, cold.reshape(1, ROWS, WIDTH)


def solution(mesh):
    return jax.shard_map(
        per_device,
        mesh=mesh,
        in_specs=(
            P(("gx", "gy")),
            P(("gx", "gy"), None),
            P("gx", "gy", None, None, None),
            P("gx", "gy", None, None),
            P("gx", "gy", None),
        ),
        out_specs=(P(), P("gx", "gy", None)),
        check_vma=False,
    )
```

```python
import jax
import jax.numpy as jnp
from jax import lax
from jax.experimental import pallas as pl
from jax.experimental.pallas import tpu as pltpu
from jax.sharding import PartitionSpec as P

MESH = pl.DeviceIdType.MESH
BF16 = jnp.bfloat16
F32 = jnp.float32

ROWS = 2048
HALF = 1024
WIDTH = 128
LOOK = 8192
CAP = 512
GX, GY, NX, NY, NZ = 8, 16, 4, 4, 4
WAVE1, WAVE2, C1, C2, C3 = 7, 10, 4, 7, 11
FACTOR = (ROWS / (LOOK * GX * GY)) ** 0.5

NEAR = sorted(
    [(a, b) for a in range(NY) for b in range(NZ)],
    key=lambda o: (min(o[0], NY - o[0]) + min(o[1], NZ - o[1]), o),
)


def selector_tile(local_ref, row, base, iota):
    halves = []
    for side in range(2):
        ids = local_ref[pl.ds(row + side, 1), :] - base
        ids = jnp.broadcast_to(ids, (16, WIDTH)).astype(BF16)
        halves.append(
            jnp.concatenate(
                [
                    jnp.where(ids == (iota + BF16(16 * i)), BF16(1), BF16(0))
                    for i in range(16)
                ],
                axis=0,
            )
        )
    return jnp.concatenate(halves, axis=1)


def split_by_bit(bits_t, column, grads):
    high = grads * jnp.broadcast_to(bits_t[:, column : column + 1], (128, WIDTH)).astype(BF16)
    return grads - high, high


def kernel(
    ids_hbm, hot_hbm, cold_hbm, slots_hbm, counts_hbm,
    hot, cold,
    ids, grads, wide, local, slots, counts, masked,
    partial, from_core, to_x, from_x, mine, from_y, got, got_slots, cold_local, cold_wide,
    local_sem, core_s, core_r, x_s, x_r, ys_s, ys_r, yg_s, yg_r,
    xg_s, xg_r, cg_s, cg_r, row_s, row_r, slot_s, slot_r,
):
    gx, gy = lax.axis_index("gx"), lax.axis_index("gy")
    x, core = gx // 2, lax.rem(gx, 2)
    y, z = gy // NZ, lax.rem(gy, NZ)

    def along_y(k):
        dy, dz = NEAR[k]
        return lax.rem(y + dy, NY) * NZ + lax.rem(z + dz, NZ)

    def x_peer(step):
        return lax.rem(x + step, NX)

    def at_gy(owner):
        return {"gx": gx, "gy": owner}

    def at_x(column):
        return {"gx": column * 2 + core, "gy": gy}

    other_core = {"gx": x * 2 + (1 - core), "gy": gy}

    def remote(src, dst, send, recv, where):
        return pltpu.make_async_remote_copy(
            src_ref=src, dst_ref=dst, send_sem=send, recv_sem=recv,
            device_id=where, device_id_type=MESH,
        )

    load_slots = pltpu.make_async_copy(slots_hbm, slots, local_sem.at[0])
    load_ids = pltpu.make_async_copy(ids_hbm, ids, local_sem.at[1])
    load_grads = pltpu.make_async_copy(hot_hbm, grads, local_sem.at[2])
    load_own = pltpu.make_async_copy(cold_hbm.at[gy], got.at[0], local_sem.at[3])
    load_counts = pltpu.make_async_copy(counts_hbm, counts, local_sem.at[4])
    load_counts.start()
    load_slots.start()
    load_ids.start()
    load_grads.start()
    load_own.start()

    barrier = pltpu.get_barrier_semaphore()
    for k in range(1, GY):
        pl.semaphore_signal(barrier, inc=1, device_id=at_gy(along_y(k)), device_id_type=MESH)
    for step in range(1, NX):
        pl.semaphore_signal(barrier, inc=1, device_id=at_x(x_peer(step)), device_id_type=MESH)
    pl.semaphore_signal(barrier, inc=1, device_id=other_core, device_id_type=MESH)

    load_slots.wait()
    load_counts.wait()
    place = lax.broadcasted_iota(jnp.int32, (1, WIDTH), 1)
    masked[...] = jnp.full_like(masked, -1)
    for d in range(GY):
        for i in range(CAP // WIDTH):
            piece = slots[d : d + 1, i * WIDTH : (i + 1) * WIDTH]
            masked[d, i : i + 1, :] = jnp.where(place + i * WIDTH < counts[0, d], piece, -1)

    load_ids.wait()
    local[...] = (ids[...] & (HALF - 1)).astype(F32)
    bits_t = jnp.transpose((ids[...] >> 10).astype(F32))
    load_grads.wait()
    for r in range(LOOK // 128):
        rows = slice(r * 128, (r + 1) * 128)
        low, high = split_by_bit(bits_t, r, grads[rows, :])
        wide[rows, 0:WIDTH] = low
        wide[rows, WIDTH:] = high

    pl.semaphore_wait(barrier, GY - 1 + NX - 1 + 1)

    def row_copy(k):
        owner = along_y(k)
        return remote(cold_hbm.at[owner], got.at[k], row_s.at[k], row_r.at[k], at_gy(owner))

    def slot_copy(k):
        owner = along_y(k)
        return remote(masked.at[owner], got_slots.at[k], slot_s.at[k], slot_r.at[k], at_gy(owner))

    for k in range(1, GY):
        slot_copy(k).start()

    def send_rows(low, high):
        for k in range(low, high):
            row_copy(k).start()

    send_rows(1, WAVE1)

    iota = lax.broadcasted_iota(jnp.int32, (16, WIDTH), 0).astype(F32).astype(BF16)

    def core_copy(s):
        return remote(
            partial.at[s, 1 - core], from_core.at[s], core_s.at[s], core_r.at[s], other_core
        )

    def x_copy(s):
        return remote(to_x.at[s], from_x.at[s], x_s.at[s], x_r.at[s], at_x(x_peer(3 - s)))

    def hot_block(s, carry):
        base = (x_peer(3 - s) * 256).astype(F32)
        total = None
        for t in range(LOOK // 256):
            product = jnp.dot(
                selector_tile(local, 2 * t, base, iota),
                wide[t * 256 : (t + 1) * 256, :],
                preferred_element_type=F32,
            )
            total = product if total is None else total + product
        partial[s, 0] = total[:, :WIDTH]
        partial[s, 1] = total[:, WIDTH:]
        core_copy(s).start()

        @pl.when(s > 0)
        def _():
            core_copy(s - 1).wait_recv()
            to_x[s - 1] = partial[s - 1, core] + from_core[s - 1]
            x_copy(s - 1).start()

        return carry

    lax.fori_loop(0, NX, hot_block, 0)

    def cold_block(k, slot_rows, first):
        cold_local[...] = jnp.where(slot_rows < 0, -1, slot_rows & (HALF - 1)).astype(F32)
        turned = jnp.transpose((slot_rows >> 10).astype(F32))
        for r in range(CAP // 128):
            rows = slice(r * 128, (r + 1) * 128)
            low, high = split_by_bit(turned, r, got[k, rows, :])
            cold_wide[rows, 0:WIDTH] = low
            cold_wide[rows, WIDTH:] = high
        for j in range(4):
            total = None
            for t in range(CAP // 256):
                product = jnp.dot(
                    selector_tile(cold_local, 2 * t, 256.0 * j, iota),
                    cold_wide[t * 256 : (t + 1) * 256, :],
                    preferred_element_type=F32,
                )
                total = product if total is None else total + product
            rows = slice(j * 256, (j + 1) * 256)
            if first:
                cold[0, rows, :] = total[:, :WIDTH]
                cold[1, rows, :] = total[:, WIDTH:]
            else:
                cold[0, rows, :] += total[:, :WIDTH]
                cold[1, rows, :] += total[:, WIDTH:]

    def cold_blocks(low, high):
        def body(k, carry):
            remote(got.at[k], got.at[k], row_s.at[k], row_r.at[k], other_core).wait_recv()
            remote(
                got_slots.at[k], got_slots.at[k], slot_s.at[k], slot_r.at[k], other_core
            ).wait_recv()
            cold_block(k, got_slots[k], False)
            return carry

        lax.fori_loop(low, high, body, 0)

    load_own.wait()
    cold_block(0, masked[gy], True)

    core_copy(3).wait_recv()
    own = partial[3, core] + from_core[3]
    for s in range(3):
        x_copy(s).wait_recv()
        own = own + from_x[s]
    mine[...] = own.reshape(GY, 16, WIDTH)

    def scatter_copy(k):
        owner = along_y(k)
        return remote(mine.at[owner], from_y.at[k], ys_s.at[k], ys_r.at[k], at_gy(owner))

    for k in range(1, GY):
        scatter_copy(k).start()
    send_rows(WAVE1, WAVE2)

    cold_blocks(1, C1)

    block = core * NX + x
    sum16 = mine[gy]
    for k in range(1, GY):
        scatter_copy(k).wait_recv()
        sum16 = sum16 + from_y[k]
    hot[block, gy] = sum16 * FACTOR

    def gather_copy(k):
        return remote(
            hot.at[block, gy], hot.at[block, gy], yg_s.at[k], yg_r.at[k], at_gy(along_y(k))
        )

    for k in range(1, GY):
        gather_copy(k).start()
    send_rows(WAVE2, GY)

    cold_blocks(C1, C2)

    for k in range(1, GY):
        gather_copy(k).wait_recv()

    def x_spread(step):
        return remote(
            hot.at[block], hot.at[block], xg_s.at[step], xg_r.at[step], at_x(x_peer(step))
        )

    def core_spread(step):
        piece = core * NX + x_peer(step)
        return remote(hot.at[piece], hot.at[piece], cg_s.at[step], cg_r.at[step], other_core)

    for step in range(1, NX):
        x_spread(step).start()
    core_spread(0).start()

    cold_blocks(C2, C3)

    for step in range(1, NX):
        x_spread(step).wait_recv()
        piece = core * NX + x_peer(NX - step)
        remote(hot.at[piece], hot.at[piece], cg_s.at[step], cg_r.at[step], other_core).start()

    cold_blocks(C3, GY)

    for step in range(NX):
        core_spread(step).wait_recv()

    for k in range(1, GY):
        slot_copy(k).wait_send()
        row_copy(k).wait_send()
        scatter_copy(k).wait_send()
        gather_copy(k).wait_send()
    for s in range(NX):
        core_copy(s).wait_send()
        core_spread(s).wait_send()
    for s in range(3):
        x_copy(s).wait_send()
        x_spread(s + 1).wait_send()


def store_tables(hot, cold, hot_out, cold_out, sem):
    copies = [
        pltpu.make_async_copy(hot, hot_out, sem.at[0]),
        pltpu.make_async_copy(cold, cold_out, sem.at[1]),
    ]
    for copy in copies:
        copy.start()
    for copy in copies:
        copy.wait()


def per_device(hot_ids, hot_grads, cold_grads, cold_slots, cold_counts):
    in_hbm = pl.BlockSpec(memory_space=pltpu.HBM)
    in_vmem = pl.BlockSpec(memory_space=pltpu.VMEM)
    dma = pltpu.SemaphoreType.DMA
    hot, cold = pl.pallas_call(
        kernel,
        name="table_grads",
        out_shape=(
            jax.ShapeDtypeStruct((GX, GY, 16, WIDTH), F32),
            jax.ShapeDtypeStruct((2, HALF, WIDTH), F32),
        ),
        in_specs=[in_hbm] * 5,
        out_specs=[in_vmem] * 2,
        scratch_shapes=[
            pltpu.VMEM((LOOK // WIDTH, WIDTH), jnp.int32),
            pltpu.VMEM((LOOK, WIDTH), BF16),
            pltpu.VMEM((LOOK, 2 * WIDTH), BF16),
            pltpu.VMEM((LOOK // WIDTH, WIDTH), F32),
            pltpu.VMEM((GY, CAP), jnp.int32),
            pltpu.SMEM((1, GY), jnp.int32),
            pltpu.VMEM((GY, 8, WIDTH), jnp.int32),
            pltpu.VMEM((NX, 2, 256, WIDTH), F32),
            pltpu.VMEM((NX, 256, WIDTH), F32),
            pltpu.VMEM((3, 256, WIDTH), F32),
            pltpu.VMEM((3, 256, WIDTH), F32),
            pltpu.VMEM((GY, 16, WIDTH), F32),
            pltpu.VMEM((GY, 16, WIDTH), F32),
            pltpu.VMEM((GY, CAP, WIDTH), BF16),
            pltpu.VMEM((GY, 8, WIDTH), jnp.int32),
            pltpu.VMEM((8, WIDTH), F32),
            pltpu.VMEM((CAP, 2 * WIDTH), BF16),
            dma((5,)),
            dma((NX,)), dma((NX,)),
            dma((3,)), dma((3,)),
            dma((GY,)), dma((GY,)),
            dma((GY,)), dma((GY,)),
            dma((NX,)), dma((NX,)),
            dma((NX,)), dma((NX,)),
            dma((GY,)), dma((GY,)),
            dma((GY,)), dma((GY,)),
        ],
        compiler_params=pltpu.CompilerParams(
            collective_id=0, has_side_effects=True, vmem_limit_bytes=48 * 2**20
        ),
    )(
        *(
            pltpu.with_memory_space_constraint(a, pltpu.HBM)
            for a in (
                hot_ids.reshape(LOOK // WIDTH, WIDTH),
                hot_grads,
                cold_grads.reshape(GY, CAP, WIDTH),
                cold_slots.reshape(GY, CAP),
                cold_counts.reshape(1, GY),
            )
        )
    )
    hot_grad, cold_grad = pl.pallas_call(
        store_tables,
        name="store_tables",
        out_shape=(
            jax.ShapeDtypeStruct((ROWS, WIDTH), F32),
            jax.ShapeDtypeStruct((1, ROWS, WIDTH), F32),
        ),
        in_specs=[in_vmem] * 2,
        out_specs=[in_hbm] * 2,
        scratch_shapes=[dma((2,))],
        compiler_params=pltpu.CompilerParams(vmem_limit_bytes=4 * 2**20),
    )(hot.reshape(ROWS, WIDTH), cold.reshape(1, ROWS, WIDTH))
    return hot_grad, cold_grad


def solution(mesh):
    return jax.shard_map(
        per_device,
        mesh=mesh,
        in_specs=(
            P(("gx", "gy")),
            P(("gx", "gy"), None),
            P("gx", "gy", None, None, None),
            P("gx", "gy", None, None),
            P("gx", "gy", None),
        ),
        out_specs=(P(), P("gx", "gy", None)),
        check_vma=False,
    )
```

```python
import jax
import jax.numpy as jnp
from jax import lax
from jax.experimental import pallas as pl
from jax.experimental.pallas import tpu as pltpu
from jax.sharding import PartitionSpec as P

MESH = pl.DeviceIdType.MESH
BF16 = jnp.bfloat16
F32 = jnp.float32

ROWS = 2048
HALF = 1024
WIDTH = 128
LOOK = 8192
CAP = 512
GX, GY, NX, NY, NZ = 8, 16, 4, 4, 4
FACTOR = (ROWS / (LOOK * GX * GY)) ** 0.5

NEAR = [(0, 0), (1, 2), (3, 2), (2, 1), (2, 3), (2, 2), (0, 1), (0, 3), (1, 0), (3, 0), (1, 1), (3, 3), (1, 3), (3, 1), (0, 2), (2, 0)]
WAVE1, WAVE2, C1, CA, C2, C3 = 6, 10, 1, 3, 6, 13


def selector_tile(local_ref, row, base, iota):
    halves = []
    for side in range(2):
        ids = local_ref[pl.ds(row + side, 1), :] - base
        ids = jnp.broadcast_to(ids, (16, WIDTH)).astype(BF16)
        halves.append(
            jnp.concatenate(
                [
                    jnp.where(ids == (iota + BF16(16 * i)), BF16(1), BF16(0))
                    for i in range(16)
                ],
                axis=0,
            )
        )
    return jnp.concatenate(halves, axis=1)


def split_by_bit(bits_t, column, grads):
    high = grads * jnp.broadcast_to(bits_t[:, column : column + 1], (128, WIDTH)).astype(BF16)
    return grads - high, high


def kernel(
    ids_hbm, hot_hbm, cold_hbm, slots_hbm, counts_hbm,
    hot, cold,
    ids, grads, wide, local, slots, counts, masked,
    partial, from_core, to_x, from_x, mine, from_y, got, got_slots, cold_local, cold_wide,
    local_sem, core_s, core_r, x_s, x_r, ys_s, ys_r, yg_s, yg_r,
    xg_s, xg_r, cg_s, cg_r, row_s, row_r, slot_s, slot_r,
):
    gx, gy = lax.axis_index("gx"), lax.axis_index("gy")
    x, core = gx // 2, lax.rem(gx, 2)
    y, z = gy // NZ, lax.rem(gy, NZ)

    def along_y(k):
        dy, dz = NEAR[k]
        return lax.rem(y + dy, NY) * NZ + lax.rem(z + dz, NZ)

    def x_peer(step):
        return lax.rem(x + step, NX)

    def x_turn(s):
        return x_peer(2 - s + s // 2 * 3 - s // 3 * 2)

    def at_gy(owner):
        return {"gx": gx, "gy": owner}

    def at_x(column):
        return {"gx": column * 2 + core, "gy": gy}

    other_core = {"gx": x * 2 + (1 - core), "gy": gy}

    def remote(src, dst, send, recv, where):
        return pltpu.make_async_remote_copy(
            src_ref=src, dst_ref=dst, send_sem=send, recv_sem=recv,
            device_id=where, device_id_type=MESH,
        )

    load_slots = pltpu.make_async_copy(slots_hbm, slots, local_sem.at[0])
    load_ids = pltpu.make_async_copy(ids_hbm, ids, local_sem.at[1])
    load_grads = pltpu.make_async_copy(hot_hbm, grads, local_sem.at[2])
    load_own = pltpu.make_async_copy(cold_hbm.at[gy], got.at[0], local_sem.at[3])
    load_counts = pltpu.make_async_copy(counts_hbm, counts, local_sem.at[4])
    load_counts.start()
    load_slots.start()
    load_ids.start()
    load_grads.start()
    load_own.start()

    barrier = pltpu.get_barrier_semaphore()
    for k in range(1, GY):
        pl.semaphore_signal(barrier, inc=1, device_id=at_gy(along_y(k)), device_id_type=MESH)
    for step in range(1, NX):
        pl.semaphore_signal(barrier, inc=1, device_id=at_x(x_peer(step)), device_id_type=MESH)
    pl.semaphore_signal(barrier, inc=1, device_id=other_core, device_id_type=MESH)

    load_slots.wait()
    load_counts.wait()
    place = lax.broadcasted_iota(jnp.int32, (1, WIDTH), 1)
    masked[...] = jnp.full_like(masked, -1)
    for d in range(GY):
        for i in range(CAP // WIDTH):
            piece = slots[d : d + 1, i * WIDTH : (i + 1) * WIDTH]
            masked[d, i : i + 1, :] = jnp.where(place + i * WIDTH < counts[0, d], piece, -1)

    load_ids.wait()
    local[...] = (ids[...] & (HALF - 1)).astype(F32)
    bits_t = jnp.transpose((ids[...] >> 10).astype(F32))
    load_grads.wait()
    for r in range(LOOK // 128):
        rows = slice(r * 128, (r + 1) * 128)
        low, high = split_by_bit(bits_t, r, grads[rows, :])
        wide[rows, 0:WIDTH] = low
        wide[rows, WIDTH:] = high

    pl.semaphore_wait(barrier, GY - 1 + NX - 1 + 1)

    def row_copy(k):
        owner = along_y(k)
        return remote(cold_hbm.at[owner], got.at[k], row_s.at[k], row_r.at[k], at_gy(owner))

    def slot_copy(k):
        owner = along_y(k)
        return remote(masked.at[owner], got_slots.at[k], slot_s.at[k], slot_r.at[k], at_gy(owner))

    for k in range(1, GY):
        slot_copy(k).start()

    def send_rows(low, high):
        for k in range(low, high):
            row_copy(k).start()

    send_rows(1, WAVE1)

    iota = lax.broadcasted_iota(jnp.int32, (16, WIDTH), 0).astype(F32).astype(BF16)

    def core_copy(s):
        return remote(
            partial.at[s, 1 - core], from_core.at[s], core_s.at[s], core_r.at[s], other_core
        )

    def x_copy(s):
        return remote(to_x.at[s], from_x.at[s], x_s.at[s], x_r.at[s], at_x(x_turn(s)))

    def hot_block(s, carry):
        base = (x_turn(s) * 256).astype(F32)
        total = None
        for t in range(LOOK // 256):
            product = jnp.dot(
                selector_tile(local, 2 * t, base, iota),
                wide[t * 256 : (t + 1) * 256, :],
                preferred_element_type=F32,
            )
            total = product if total is None else total + product
        partial[s, 0] = total[:, :WIDTH]
        partial[s, 1] = total[:, WIDTH:]
        core_copy(s).start()

        @pl.when(s > 0)
        def _():
            core_copy(s - 1).wait_recv()
            to_x[s - 1] = partial[s - 1, core] + from_core[s - 1]
            x_copy(s - 1).start()

        return carry

    lax.fori_loop(0, NX, hot_block, 0)

    def cold_block(k, slot_rows, first):
        cold_local[...] = jnp.where(slot_rows < 0, -1, slot_rows & (HALF - 1)).astype(F32)
        turned = jnp.transpose((slot_rows >> 10).astype(F32))
        for r in range(CAP // 128):
            rows = slice(r * 128, (r + 1) * 128)
            low, high = split_by_bit(turned, r, got[k, rows, :])
            cold_wide[rows, 0:WIDTH] = low
            cold_wide[rows, WIDTH:] = high
        for j in range(4):
            total = None
            for t in range(CAP // 256):
                product = jnp.dot(
                    selector_tile(cold_local, 2 * t, 256.0 * j, iota),
                    cold_wide[t * 256 : (t + 1) * 256, :],
                    preferred_element_type=F32,
                )
                total = product if total is None else total + product
            rows = slice(j * 256, (j + 1) * 256)
            if first:
                cold[0, rows, :] = total[:, :WIDTH]
                cold[1, rows, :] = total[:, WIDTH:]
            else:
                cold[0, rows, :] += total[:, :WIDTH]
                cold[1, rows, :] += total[:, WIDTH:]

    def cold_blocks(low, high):
        def body(k, carry):
            remote(got.at[k], got.at[k], row_s.at[k], row_r.at[k], other_core).wait_recv()
            remote(
                got_slots.at[k], got_slots.at[k], slot_s.at[k], slot_r.at[k], other_core
            ).wait_recv()
            cold_block(k, got_slots[k], False)
            return carry

        lax.fori_loop(low, high, body, 0)

    load_own.wait()
    cold_block(0, masked[gy], True)

    core_copy(3).wait_recv()
    own = partial[3, core] + from_core[3]
    for s in range(3):
        x_copy(s).wait_recv()
        own = own + from_x[s]
    mine[...] = own.reshape(GY, 16, WIDTH)

    def scatter_copy(k):
        owner = along_y(k)
        return remote(mine.at[owner], from_y.at[k], ys_s.at[k], ys_r.at[k], at_gy(owner))

    for k in range(1, GY):
        scatter_copy(k).start()
    send_rows(WAVE1, WAVE2)

    cold_blocks(1, C1)

    block = core * NX + x
    sum16 = mine[gy]
    for k in range(1, GY):
        scatter_copy(k).wait_recv()
        sum16 = sum16 + from_y[k]
    hot[block, gy] = sum16 * FACTOR

    def gather_copy(k):
        return remote(
            hot.at[block, gy], hot.at[block, gy], yg_s.at[k], yg_r.at[k], at_gy(along_y(k))
        )

    for k in range(1, GY):
        gather_copy(k).start()
    cold_blocks(C1, CA)
    send_rows(WAVE2, GY)
    cold_blocks(CA, C2)

    for k in range(1, GY):
        gather_copy(k).wait_recv()

    def x_spread(step):
        return remote(
            hot.at[block], hot.at[block], xg_s.at[step], xg_r.at[step], at_x(x_peer(step))
        )

    def core_spread(step):
        piece = core * NX + x_peer(step)
        return remote(hot.at[piece], hot.at[piece], cg_s.at[step], cg_r.at[step], other_core)

    for step in range(1, NX):
        x_spread(step).start()
    core_spread(0).start()

    cold_blocks(C2, C3)

    for step in range(1, NX):
        x_spread(step).wait_recv()
        piece = core * NX + x_peer(NX - step)
        remote(hot.at[piece], hot.at[piece], cg_s.at[step], cg_r.at[step], other_core).start()

    cold_blocks(C3, GY)

    for step in range(NX):
        core_spread(step).wait_recv()

    for k in range(1, GY):
        slot_copy(k).wait_send()
        row_copy(k).wait_send()
        scatter_copy(k).wait_send()
        gather_copy(k).wait_send()
    for s in range(NX):
        core_copy(s).wait_send()
        core_spread(s).wait_send()
    for s in range(3):
        x_copy(s).wait_send()
        x_spread(s + 1).wait_send()


def store_tables(hot, cold, hot_out, cold_out, sem):
    copies = [
        pltpu.make_async_copy(hot, hot_out, sem.at[0]),
        pltpu.make_async_copy(cold, cold_out, sem.at[1]),
    ]
    for copy in copies:
        copy.start()
    for copy in copies:
        copy.wait()


def per_device(hot_ids, hot_grads, cold_grads, cold_slots, cold_counts):
    in_hbm = pl.BlockSpec(memory_space=pltpu.HBM)
    in_vmem = pl.BlockSpec(memory_space=pltpu.VMEM)
    dma = pltpu.SemaphoreType.DMA
    hot, cold = pl.pallas_call(
        kernel,
        name="table_grads",
        out_shape=(
            jax.ShapeDtypeStruct((GX, GY, 16, WIDTH), F32),
            jax.ShapeDtypeStruct((2, HALF, WIDTH), F32),
        ),
        in_specs=[in_hbm] * 5,
        out_specs=[in_vmem] * 2,
        scratch_shapes=[
            pltpu.VMEM((LOOK // WIDTH, WIDTH), jnp.int32),
            pltpu.VMEM((LOOK, WIDTH), BF16),
            pltpu.VMEM((LOOK, 2 * WIDTH), BF16),
            pltpu.VMEM((LOOK // WIDTH, WIDTH), F32),
            pltpu.VMEM((GY, CAP), jnp.int32),
            pltpu.SMEM((1, GY), jnp.int32),
            pltpu.VMEM((GY, 8, WIDTH), jnp.int32),
            pltpu.VMEM((NX, 2, 256, WIDTH), F32),
            pltpu.VMEM((NX, 256, WIDTH), F32),
            pltpu.VMEM((3, 256, WIDTH), F32),
            pltpu.VMEM((3, 256, WIDTH), F32),
            pltpu.VMEM((GY, 16, WIDTH), F32),
            pltpu.VMEM((GY, 16, WIDTH), F32),
            pltpu.VMEM((GY, CAP, WIDTH), BF16),
            pltpu.VMEM((GY, 8, WIDTH), jnp.int32),
            pltpu.VMEM((8, WIDTH), F32),
            pltpu.VMEM((CAP, 2 * WIDTH), BF16),
            dma((5,)),
            dma((NX,)), dma((NX,)),
            dma((3,)), dma((3,)),
            dma((GY,)), dma((GY,)),
            dma((GY,)), dma((GY,)),
            dma((NX,)), dma((NX,)),
            dma((NX,)), dma((NX,)),
            dma((GY,)), dma((GY,)),
            dma((GY,)), dma((GY,)),
        ],
        compiler_params=pltpu.CompilerParams(
            collective_id=0, has_side_effects=True, vmem_limit_bytes=48 * 2**20
        ),
    )(
        *(
            pltpu.with_memory_space_constraint(a, pltpu.HBM)
            for a in (
                hot_ids.reshape(LOOK // WIDTH, WIDTH),
                hot_grads,
                cold_grads.reshape(GY, CAP, WIDTH),
                cold_slots.reshape(GY, CAP),
                cold_counts.reshape(1, GY),
            )
        )
    )
    hot_grad, cold_grad = pl.pallas_call(
        store_tables,
        name="store_tables",
        out_shape=(
            jax.ShapeDtypeStruct((ROWS, WIDTH), F32),
            jax.ShapeDtypeStruct((1, ROWS, WIDTH), F32),
        ),
        in_specs=[in_vmem] * 2,
        out_specs=[in_hbm] * 2,
        scratch_shapes=[dma((2,))],
        compiler_params=pltpu.CompilerParams(vmem_limit_bytes=4 * 2**20),
    )(hot.reshape(ROWS, WIDTH), cold.reshape(1, ROWS, WIDTH))
    return hot_grad, cold_grad


def solution(mesh):
    return jax.shard_map(
        per_device,
        mesh=mesh,
        in_specs=(
            P(("gx", "gy")),
            P(("gx", "gy"), None),
            P("gx", "gy", None, None, None),
            P("gx", "gy", None, None),
            P("gx", "gy", None),
        ),
        out_specs=(P(), P("gx", "gy", None)),
        check_vma=False,
    )
```

```python
import jax
import jax.numpy as jnp
from jax import lax
from jax.experimental import pallas as pl
from jax.experimental.pallas import tpu as pltpu
from jax.sharding import PartitionSpec as P

MESH = pl.DeviceIdType.MESH
BF16 = jnp.bfloat16
F32 = jnp.float32

ROWS = 2048
HALF = 1024
WIDTH = 128
LOOK = 8192
CAP = 512
GX, GY, NX, NY, NZ = 8, 16, 4, 4, 4
FACTOR = (ROWS / (LOOK * GX * GY)) ** 0.5

NEAR = [(0, 0), (1, 2), (3, 2), (2, 1), (2, 3), (2, 2), (0, 1), (0, 3), (1, 0), (3, 0), (1, 1), (3, 3), (1, 3), (3, 1), (0, 2), (2, 0)]
WAVE1, WAVE2, C1, CA, C2, C3 = 6, 10, 1, 5, 6, 14


def selector_tile(local_ref, row, base, iota):
    halves = []
    for side in range(2):
        ids = local_ref[pl.ds(row + side, 1), :] - base
        ids = jnp.broadcast_to(ids, (16, WIDTH)).astype(BF16)
        halves.append(
            jnp.concatenate(
                [
                    jnp.where(ids == (iota + BF16(16 * i)), BF16(1), BF16(0))
                    for i in range(16)
                ],
                axis=0,
            )
        )
    return jnp.concatenate(halves, axis=1)


def split_by_bit(bits_t, column, grads):
    high = grads * jnp.broadcast_to(bits_t[:, column : column + 1], (128, WIDTH)).astype(BF16)
    return grads - high, high


def kernel(
    ids_hbm, hot_hbm, cold_hbm, slots_hbm, counts_hbm,
    hot, cold,
    ids, grads, wide, local, slots, counts, masked,
    partial, from_core, to_x, from_x, mine, from_y, got, got_slots, cold_local, cold_wide,
    local_sem, core_s, core_r, x_s, x_r, ys_s, ys_r, yg_s, yg_r,
    xg_s, xg_r, cg_s, cg_r, row_s, row_r, slot_s, slot_r,
):
    gx, gy = lax.axis_index("gx"), lax.axis_index("gy")
    x, core = gx // 2, lax.rem(gx, 2)
    y, z = gy // NZ, lax.rem(gy, NZ)

    def along_y(k):
        dy, dz = NEAR[k]
        return lax.rem(y + dy, NY) * NZ + lax.rem(z + dz, NZ)

    def x_peer(step):
        return lax.rem(x + step, NX)

    def x_turn(s):
        return x_peer(2 - s + s // 2 * 3 - s // 3 * 2)

    def at_gy(owner):
        return {"gx": gx, "gy": owner}

    def at_x(column):
        return {"gx": column * 2 + core, "gy": gy}

    other_core = {"gx": x * 2 + (1 - core), "gy": gy}

    def remote(src, dst, send, recv, where):
        return pltpu.make_async_remote_copy(
            src_ref=src, dst_ref=dst, send_sem=send, recv_sem=recv,
            device_id=where, device_id_type=MESH,
        )

    load_slots = pltpu.make_async_copy(slots_hbm, slots, local_sem.at[0])
    load_ids = pltpu.make_async_copy(ids_hbm, ids, local_sem.at[1])
    load_grads = pltpu.make_async_copy(hot_hbm, grads, local_sem.at[2])
    load_own = pltpu.make_async_copy(cold_hbm.at[gy], got.at[0], local_sem.at[3])
    load_counts = pltpu.make_async_copy(counts_hbm, counts, local_sem.at[4])
    load_counts.start()
    load_slots.start()
    load_ids.start()
    load_grads.start()
    load_own.start()

    barrier = pltpu.get_barrier_semaphore()
    for k in range(1, GY):
        pl.semaphore_signal(barrier, inc=1, device_id=at_gy(along_y(k)), device_id_type=MESH)
    for step in range(1, NX):
        pl.semaphore_signal(barrier, inc=1, device_id=at_x(x_peer(step)), device_id_type=MESH)
    pl.semaphore_signal(barrier, inc=1, device_id=other_core, device_id_type=MESH)

    load_slots.wait()
    load_counts.wait()
    place = lax.broadcasted_iota(jnp.int32, (1, WIDTH), 1)
    masked[...] = jnp.full_like(masked, -1)
    for d in range(GY):
        for i in range(CAP // WIDTH):
            piece = slots[d : d + 1, i * WIDTH : (i + 1) * WIDTH]
            masked[d, i : i + 1, :] = jnp.where(place + i * WIDTH < counts[0, d], piece, -1)

    load_ids.wait()
    local[...] = (ids[...] & (HALF - 1)).astype(F32)
    bits_t = jnp.transpose((ids[...] >> 10).astype(F32))
    load_grads.wait()
    for r in range(LOOK // 128):
        rows = slice(r * 128, (r + 1) * 128)
        low, high = split_by_bit(bits_t, r, grads[rows, :])
        wide[rows, 0:WIDTH] = low
        wide[rows, WIDTH:] = high

    pl.semaphore_wait(barrier, GY - 1 + NX - 1 + 1)

    def row_copy(k):
        owner = along_y(k)
        return remote(cold_hbm.at[owner], got.at[k], row_s.at[k], row_r.at[k], at_gy(owner))

    def slot_copy(k):
        owner = along_y(k)
        return remote(masked.at[owner], got_slots.at[k], slot_s.at[k], slot_r.at[k], at_gy(owner))

    for k in range(1, GY):
        slot_copy(k).start()

    def send_rows(low, high):
        for k in range(low, high):
            row_copy(k).start()

    send_rows(1, WAVE1)

    iota = lax.broadcasted_iota(jnp.int32, (16, WIDTH), 0).astype(F32).astype(BF16)

    def core_copy(s):
        return remote(
            partial.at[s, 1 - core], from_core.at[s], core_s.at[s], core_r.at[s], other_core
        )

    def x_copy(s):
        return remote(to_x.at[s], from_x.at[s], x_s.at[s], x_r.at[s], at_x(x_turn(s)))

    def hot_block(s, carry):
        base = (x_turn(s) * 256).astype(F32)
        total = None
        for t in range(LOOK // 256):
            product = jnp.dot(
                selector_tile(local, 2 * t, base, iota),
                wide[t * 256 : (t + 1) * 256, :],
                preferred_element_type=F32,
            )
            total = product if total is None else total + product
        partial[s, 0] = total[:, :WIDTH]
        partial[s, 1] = total[:, WIDTH:]
        core_copy(s).start()

        @pl.when(s > 0)
        def _():
            core_copy(s - 1).wait_recv()
            to_x[s - 1] = partial[s - 1, core] + from_core[s - 1]
            x_copy(s - 1).start()

        return carry

    lax.fori_loop(0, NX, hot_block, 0)

    def cold_block(k, slot_rows, first):
        cold_local[...] = jnp.where(slot_rows < 0, -1, slot_rows & (HALF - 1)).astype(F32)
        turned = jnp.transpose((slot_rows >> 10).astype(F32))
        for r in range(CAP // 128):
            rows = slice(r * 128, (r + 1) * 128)
            low, high = split_by_bit(turned, r, got[k, rows, :])
            cold_wide[rows, 0:WIDTH] = low
            cold_wide[rows, WIDTH:] = high
        for j in range(4):
            total = None
            for t in range(CAP // 256):
                product = jnp.dot(
                    selector_tile(cold_local, 2 * t, 256.0 * j, iota),
                    cold_wide[t * 256 : (t + 1) * 256, :],
                    preferred_element_type=F32,
                )
                total = product if total is None else total + product
            rows = slice(j * 256, (j + 1) * 256)
            if first:
                cold[0, rows, :] = total[:, :WIDTH]
                cold[1, rows, :] = total[:, WIDTH:]
            else:
                cold[0, rows, :] += total[:, :WIDTH]
                cold[1, rows, :] += total[:, WIDTH:]

    def cold_blocks(low, high):
        def body(k, carry):
            remote(got.at[k], got.at[k], row_s.at[k], row_r.at[k], other_core).wait_recv()
            remote(
                got_slots.at[k], got_slots.at[k], slot_s.at[k], slot_r.at[k], other_core
            ).wait_recv()
            cold_block(k, got_slots[k], False)
            return carry

        lax.fori_loop(low, high, body, 0)

    load_own.wait()
    cold_block(0, masked[gy], True)

    core_copy(3).wait_recv()
    own = partial[3, core] + from_core[3]
    for s in range(3):
        x_copy(s).wait_recv()
        own = own + from_x[s]
    mine[...] = own.reshape(GY, 16, WIDTH)

    def scatter_copy(k):
        owner = along_y(k)
        return remote(mine.at[owner], from_y.at[k], ys_s.at[k], ys_r.at[k], at_gy(owner))

    for k in range(1, GY):
        scatter_copy(k).start()
    send_rows(WAVE1, WAVE2)

    cold_blocks(1, C1)

    block = core * NX + x
    sum16 = mine[gy]
    for k in range(1, GY):
        scatter_copy(k).wait_recv()
        sum16 = sum16 + from_y[k]
    hot[block, gy] = sum16 * FACTOR

    def gather_copy(k):
        return remote(
            hot.at[block, gy], hot.at[block, gy], yg_s.at[k], yg_r.at[k], at_gy(along_y(k))
        )

    for k in range(1, GY):
        gather_copy(k).start()
    cold_blocks(C1, CA)
    send_rows(WAVE2, GY)
    cold_blocks(CA, C2)

    for k in range(1, GY):
        gather_copy(k).wait_recv()

    def x_spread(step):
        return remote(
            hot.at[block], hot.at[block], xg_s.at[step], xg_r.at[step], at_x(x_peer(step))
        )

    def core_spread(step):
        piece = core * NX + x_peer(step)
        return remote(hot.at[piece], hot.at[piece], cg_s.at[step], cg_r.at[step], other_core)

    for step in (2, 1, 3):
        x_spread(step).start()
    core_spread(0).start()

    cold_blocks(C2, C3)

    for step in (1, 3, 2):
        x_spread(step).wait_recv()
        piece = core * NX + x_peer(NX - step)
        remote(hot.at[piece], hot.at[piece], cg_s.at[step], cg_r.at[step], other_core).start()

    cold_blocks(C3, GY)

    for step in range(NX):
        core_spread(step).wait_recv()

    for k in range(1, GY):
        slot_copy(k).wait_send()
        row_copy(k).wait_send()
        scatter_copy(k).wait_send()
        gather_copy(k).wait_send()
    for s in range(NX):
        core_copy(s).wait_send()
        core_spread(s).wait_send()
    for s in range(3):
        x_copy(s).wait_send()
        x_spread(s + 1).wait_send()


def store_tables(hot, cold, hot_out, cold_out, sem):
    copies = [
        pltpu.make_async_copy(hot, hot_out, sem.at[0]),
        pltpu.make_async_copy(cold, cold_out, sem.at[1]),
    ]
    for copy in copies:
        copy.start()
    for copy in copies:
        copy.wait()


def per_device(hot_ids, hot_grads, cold_grads, cold_slots, cold_counts):
    in_hbm = pl.BlockSpec(memory_space=pltpu.HBM)
    in_vmem = pl.BlockSpec(memory_space=pltpu.VMEM)
    dma = pltpu.SemaphoreType.DMA
    hot, cold = pl.pallas_call(
        kernel,
        name="table_grads",
        out_shape=(
            jax.ShapeDtypeStruct((GX, GY, 16, WIDTH), F32),
            jax.ShapeDtypeStruct((2, HALF, WIDTH), F32),
        ),
        in_specs=[in_hbm] * 5,
        out_specs=[in_vmem] * 2,
        scratch_shapes=[
            pltpu.VMEM((LOOK // WIDTH, WIDTH), jnp.int32),
            pltpu.VMEM((LOOK, WIDTH), BF16),
            pltpu.VMEM((LOOK, 2 * WIDTH), BF16),
            pltpu.VMEM((LOOK // WIDTH, WIDTH), F32),
            pltpu.VMEM((GY, CAP), jnp.int32),
            pltpu.SMEM((1, GY), jnp.int32),
            pltpu.VMEM((GY, 8, WIDTH), jnp.int32),
            pltpu.VMEM((NX, 2, 256, WIDTH), F32),
            pltpu.VMEM((NX, 256, WIDTH), F32),
            pltpu.VMEM((3, 256, WIDTH), F32),
            pltpu.VMEM((3, 256, WIDTH), F32),
            pltpu.VMEM((GY, 16, WIDTH), F32),
            pltpu.VMEM((GY, 16, WIDTH), F32),
            pltpu.VMEM((GY, CAP, WIDTH), BF16),
            pltpu.VMEM((GY, 8, WIDTH), jnp.int32),
            pltpu.VMEM((8, WIDTH), F32),
            pltpu.VMEM((CAP, 2 * WIDTH), BF16),
            dma((5,)),
            dma((NX,)), dma((NX,)),
            dma((3,)), dma((3,)),
            dma((GY,)), dma((GY,)),
            dma((GY,)), dma((GY,)),
            dma((NX,)), dma((NX,)),
            dma((NX,)), dma((NX,)),
            dma((GY,)), dma((GY,)),
            dma((GY,)), dma((GY,)),
        ],
        compiler_params=pltpu.CompilerParams(
            collective_id=0, has_side_effects=True, vmem_limit_bytes=48 * 2**20
        ),
    )(
        *(
            pltpu.with_memory_space_constraint(a, pltpu.HBM)
            for a in (
                hot_ids.reshape(LOOK // WIDTH, WIDTH),
                hot_grads,
                cold_grads.reshape(GY, CAP, WIDTH),
                cold_slots.reshape(GY, CAP),
                cold_counts.reshape(1, GY),
            )
        )
    )
    hot_grad, cold_grad = pl.pallas_call(
        store_tables,
        name="store_tables",
        out_shape=(
            jax.ShapeDtypeStruct((ROWS, WIDTH), F32),
            jax.ShapeDtypeStruct((1, ROWS, WIDTH), F32),
        ),
        in_specs=[in_vmem] * 2,
        out_specs=[in_hbm] * 2,
        scratch_shapes=[dma((2,))],
        compiler_params=pltpu.CompilerParams(vmem_limit_bytes=4 * 2**20),
    )(hot.reshape(ROWS, WIDTH), cold.reshape(1, ROWS, WIDTH))
    return hot_grad, cold_grad


def solution(mesh):
    return jax.shard_map(
        per_device,
        mesh=mesh,
        in_specs=(
            P(("gx", "gy")),
            P(("gx", "gy"), None),
            P("gx", "gy", None, None, None),
            P("gx", "gy", None, None),
            P("gx", "gy", None),
        ),
        out_specs=(P(), P("gx", "gy", None)),
        check_vma=False,
    )
```
